256 devices in a mesh: row: 16 (over z, x_lo), col: 4 (over y), mode: 4 (over x_hi, core).
Axes of the slice: x: 4 (x_hi: 2, x_lo: 2; x = x_hi * 2 + x_lo), y: 4, z: 8, core: 2. Of those that a mesh axis runs over, the one named last changes fastest.
Arguments:
- object_field: float32 [2, 4096, 1024], P(None, 'row', 'col'), may hold values from -6 to 6
- probe_real: float32 [4, 128, 128], P('mode'), may hold values from -3 to 3
- probe_imag: float32 [4, 128, 128], P('mode'), may hold values from -3 to 3
- amplitude: float32 [16, 4, 8, 128, 128], P('row', 'col'), may hold values from 0 to 3
- positions: int32 [16, 4, 8, 2], P('row', 'col'), may hold values from 0 to 256, as said below
- counts: int32 [16, 4], P('row', 'col'), may hold values from 2 to 8, as said below
Outputs:
- updated: float32 [2, 4096, 1024], P(None, 'row', 'col')
The draws below stay inside these ranges and needn't reach their ends.
Inputs may be any that keep to these rules, and one draw needn't show every extreme that they name: `positions`: offsets lie in 0 to 256 for rows and 0 to 256 for columns. In every tile slot 0 starts within the first 64 rows and columns of the window, and slot 1 ends within the last 64 rows and columns. `counts`: some tile has 8 frames and some tile has 2.
All inputs are finite; a program needn't handle non-finite values.
Results may differ from the reference program's by a relative error of at most 0.0003.
Values sent between devices are 32-bit elements; how exact they have to be, the bound alone decides.
No kernel may reach another device: no remote copies, remote signals or barrier semaphores. Data moves between devices by JAX's collectives and lax.ppermute only.
A program may use at most 64 MiB of HBM per device.

```python
import jax
import jax.numpy as jnp
from jax import lax

FRAME = 128
MARGIN = 64
SLOTS = 8
TH = 256
TW = 256
MODES = 4
NH = 4096
NW = 1024
N_ROW = 16
N_COL = 4


def draw_positions(key, part):
    tiles = NH // TH * (NW // TW)
    span_rows = TH + 2 * MARGIN - FRAME
    span_cols = TW + 2 * MARGIN - FRAME
    keys = jax.random.split(jax.random.fold_in(key, 11), 6)
    rows = jax.random.randint(keys[0], (tiles, SLOTS), 0, span_rows + 1)
    cols = jax.random.randint(keys[1], (tiles, SLOTS), 0, span_cols + 1)
    rows = rows.at[:, 0].set(jax.random.randint(keys[2], (tiles,), 0, MARGIN))
    cols = cols.at[:, 0].set(jax.random.randint(keys[3], (tiles,), 0, MARGIN))
    rows = rows.at[:, 1].set(jax.random.randint(keys[4], (tiles,), span_rows - MARGIN + 1, span_rows + 1))
    cols = cols.at[:, 1].set(jax.random.randint(keys[5], (tiles,), span_cols - MARGIN + 1, span_cols + 1))
    stacked = jnp.stack([rows, cols], axis=-1).astype(jnp.int32)
    return stacked.reshape(NH // TH, NW // TW, SLOTS, 2)


def draw_counts(key, part):
    tiles = NH // TH * (NW // TW)
    keys = jax.random.split(jax.random.fold_in(key, 23), 3)
    first = jax.random.randint(keys[0], (tiles,), 0, SLOTS - 1)
    second = jax.random.randint(keys[1], (tiles,), 0, SLOTS - 1)
    values = 2 + jnp.minimum(first, second)
    chosen = jax.random.randint(keys[2], (), 0, tiles)
    values = values.at[chosen].set(SLOTS)
    values = values.at[(chosen + 1) % tiles].set(2)
    return values.astype(jnp.int32).reshape(NH // TH, NW // TW)


def block_scale(key, dims, cuts, smallest, top_value):
    def one(dim, parts):
        heights = jax.random.uniform(jax.random.fold_in(jax.random.fold_in(key, 6), dim), (parts,), jnp.float32, smallest / len(cuts), top_value / len(cuts))
        return jnp.repeat(jnp.exp(heights), dims[dim] // parts).reshape((-1,) + (1,) * (len(dims) - dim - 1))

    gain = one(*cuts[0])
    for cut in cuts[1:]:
        gain = gain * one(*cut)
    return gain


def noise(rng, extent, deviation, limit, pieces=(), kind=jnp.bfloat16):
    result = deviation * jax.random.normal(rng, extent, jnp.float32)
    if pieces:
        result = result * block_scale(rng, extent, pieces, -0.22, 0.18)
    return jnp.clip(result, -limit, limit).astype(kind)


def setup_inputs(seed: int = 0) -> dict:
    key_of = jax.random.split(jax.random.key(seed), 7)
    object_field = noise(key_of[0], (2, NH, NW), 1.0, 6.0, ((1, 16), (2, 4)), jnp.float32)
    probe_real = noise(key_of[1], (MODES, FRAME, FRAME), 0.5, 3.0, ((0, 4),), jnp.float32)
    probe_imag = noise(key_of[2], (MODES, FRAME, FRAME), 0.5, 3.0, ((0, 4),), jnp.float32)
    amplitude = jnp.clip(3.0 * jax.random.uniform(key_of[3], (N_ROW, N_COL, SLOTS, FRAME, FRAME), jnp.float32) ** block_scale(key_of[3], (N_ROW, N_COL, SLOTS, FRAME, FRAME), ((0, 16), (1, 4)), -0.2, 0.2), 0.0, 3.0)
    positions = draw_positions(jax.random.fold_in(key_of[6], 71), 0)
    counts = draw_counts(jax.random.fold_in(key_of[6], 71), 0)
    return {"object_field": object_field, "probe_real": probe_real, "probe_imag": probe_imag, "amplitude": amplitude, "positions": positions, "counts": counts}


STEP_SIZE = 0.25

def reference(object_field, probe_real, probe_imag, amplitude, positions, counts):
    ext_rows = TH + 2 * MARGIN
    ext_cols = TW + 2 * MARGIN
    padded = jnp.pad(object_field, ((0, 0), (MARGIN, MARGIN), (MARGIN, MARGIN)))
    probe = lax.complex(probe_real, probe_imag)
    anchor = jnp.zeros((), jnp.int32)

    def frame_grad(window, offset, target):
        patch = lax.dynamic_slice(window, (anchor, offset[0], offset[1]), (2, FRAME, FRAME))
        exit_wave = probe * lax.complex(patch[0], patch[1])
        spectra = jnp.fft.fft2(exit_wave, norm='ortho')
        intensity = lax.optimization_barrier(jnp.sum(jnp.real(spectra) ** 2 + jnp.imag(spectra) ** 2, axis=0))
        keep = 1.0 - target / jnp.maximum(jnp.sqrt(intensity), 1.0)
        back = jnp.fft.ifft2(spectra * keep, norm='ortho')
        contrib = lax.optimization_barrier(jnp.sum(jnp.conj(probe) * back, axis=0))
        return jnp.stack([jnp.real(contrib), jnp.imag(contrib)])

    def tile_step(gradient, index):
        row_tile = index // N_COL
        col_tile = index % N_COL
        start = (anchor, row_tile * TH, col_tile * TW)
        window = lax.dynamic_slice(padded, start, (2, ext_rows, ext_cols))
        local = jnp.zeros((2, ext_rows, ext_cols), padded.dtype)

        def slot_step(slot, local):
            offset = positions[row_tile, col_tile, slot].astype(jnp.int32)
            weight = (slot < counts[row_tile, col_tile]).astype(padded.dtype)
            piece = frame_grad(window, offset, amplitude[row_tile, col_tile, slot]) * weight
            corner = (anchor, offset[0], offset[1])
            previous = lax.dynamic_slice(local, corner, (2, FRAME, FRAME))
            return lax.dynamic_update_slice(local, previous + piece, corner)
        local = lax.fori_loop(0, SLOTS, slot_step, local)
        previous = lax.dynamic_slice(gradient, start, (2, ext_rows, ext_cols))
        return (lax.dynamic_update_slice(gradient, previous + local, start), None)
    gradient, _ = lax.scan(tile_step, jnp.zeros(padded.shape, padded.dtype), jnp.arange(N_ROW * N_COL, dtype=jnp.int32))
    cropped = gradient[:, MARGIN:MARGIN + NH, MARGIN:MARGIN + NW]
    return object_field - STEP_SIZE * cropped
```

```python
import jax
import jax.numpy as jnp
import ml_dtypes
import numpy as np
from jax import lax
from jax.experimental import pallas as pl
from jax.experimental.pallas import tpu as pltpu
from jax.sharding import PartitionSpec as P

FRAME = 128
MARGIN = 64
SLOTS = 8
MODES = 4
TILE = 256
WINDOW = TILE + 2 * MARGIN
STEP_SIZE = 0.25
AXES = ("row", "col", "mode")
F32 = jnp.float32
BF16 = jnp.bfloat16


def dft_tables():
    n = np.arange(FRAME)
    angle = 2.0 * np.pi * ((n[:, None] * n[None, :]) % FRAME) / FRAME
    cosine, sine = np.cos(angle), np.sin(angle)
    right = np.block([[cosine, -sine], [sine, cosine]])
    left = right.T / FRAME

    def halves(table):
        table = table.astype(np.float32)
        high = table.astype(ml_dtypes.bfloat16)
        low = (table - high.astype(np.float32)).astype(ml_dtypes.bfloat16)
        return high, low

    return np.stack(halves(right) + halves(left))


def partner(kind, index, count):
    if kind == 0:
        return index
    if kind == 1:
        return index ^ 1
    return (((index + 1) ^ 1) - 1) % count if index else count - 1


def swap(x, mesh_shape, by_core):
    rows, cols, modes = (mesh_shape[a] for a in AXES)
    pairs = []
    for r in range(rows):
        for c in range(cols):
            for m in range(modes):
                row_kind, col_kind, flip = by_core[m % 2]
                rr, cc = partner(row_kind, r, rows), partner(col_kind, c, cols)
                pairs.append(((r * cols + c) * modes + m, (rr * cols + cc) * modes + (m ^ flip)))
    return lax.ppermute(x, AXES, pairs)


def lanes_below(shape):
    return lax.broadcasted_iota(jnp.int32, shape, len(shape) - 1) < MARGIN


def directions():
    r, c, k = lax.axis_index("row"), lax.axis_index("col"), lax.axis_index("mode") % 2
    down = (r + k) % 2 == 0
    right = (c + k) % 2 == 0
    return r, c, down, right


def packed(real, imag, lower):
    low = lanes_below(real.shape)
    natural = low == lower
    return jnp.where(natural, real, pltpu.roll(imag, MARGIN, 1))


def pack_kernel(obj, pr, pi, row_o, col_o, c1_o, c2_o, probe_o):
    _, _, down, right = directions()
    start = pl.multiple_of(jnp.where(down, TILE - MARGIN, 0), MARGIN)
    for ri in range(2):
        for blk in range(2):
            row_o[pl.ds((ri * 2 + blk) * MARGIN, MARGIN), :] = obj[ri, pl.ds(start, MARGIN), pl.ds(blk * 128, 128)]

    def side(rows, to_right):
        real = jnp.where(to_right, obj[0, rows, 128:256], obj[0, rows, 0:128])
        imag = jnp.where(to_right, obj[1, rows, 128:256], obj[1, rows, 0:128])
        return packed(real, imag, jnp.logical_not(to_right))

    col_o[...] = side(slice(None), right)
    c1_o[...] = side(pl.ds(start, MARGIN), right)
    c2_o[...] = side(pl.ds(start, MARGIN), jnp.logical_not(right))
    probe_o[0:128, :] = pr[0]
    probe_o[128:256, :] = pi[0]


def put_split(high, low, rows, cols, value):
    h = value.astype(BF16)
    high[rows, cols] = h
    low[rows, cols] = (value - h.astype(F32)).astype(BF16)


def main_kernel(
    pos, cnt, obj, row_i, col_i, c1_i, c2_i, probe_i, xprobe_i, pprobe_i, both_i, amp, tab,
    part_o, row_o, col_o, c1_o, c2_o,
    ext, grad, probes, s1h, s1l, s2h, s2l, zs, s3h, s3l, s4h, s4l,
):
    r, c, down, right = directions()
    member = lax.axis_index("mode")
    rows_count, cols_count = lax.axis_size("row"), lax.axis_size("col")
    ok_down, ok_up = r < rows_count - 1, r > 0
    ok_right, ok_left = c < cols_count - 1, c > 0

    probes[member] = probe_i[...]
    probes[member ^ 2] = xprobe_i[...]
    probes[member ^ 1] = pprobe_i[...]
    probes[member ^ 3] = both_i[pl.ds(640, 256), :]

    for ri in range(2):
        for blk in range(2):
            ext[ri, blk, MARGIN : MARGIN + TILE, :] = obj[ri, :, blk * 128 : (blk + 1) * 128]
    own_rows = pl.multiple_of(jnp.where(down, MARGIN + TILE, 0), MARGIN)
    other_rows = pl.multiple_of(jnp.where(down, 0, MARGIN + TILE), MARGIN)
    ok_own = jnp.where(down, ok_down, ok_up)
    ok_other = jnp.where(down, ok_up, ok_down)
    for ri in range(2):
        for blk in range(2):
            at = (ri * 2 + blk) * MARGIN
            ext[ri, blk, pl.ds(own_rows, MARGIN), :] = jnp.where(ok_own, row_i[at : at + MARGIN, :], 0.0)
            ext[ri, blk, pl.ds(other_rows, MARGIN), :] = jnp.where(ok_other, both_i[at : at + MARGIN, :], 0.0)

    def put_side(rows, from_right, from_left, ok):
        low = lanes_below(from_right.shape)
        from_right = jnp.where(jnp.logical_and(ok, ok_right), from_right, 0.0)
        from_left = jnp.where(jnp.logical_and(ok, ok_left), from_left, 0.0)
        ext[0, 2, rows, :] = jnp.where(low, from_right, from_left)
        ext[1, 2, rows, :] = pltpu.roll(jnp.where(low, from_left, from_right), MARGIN, 1)

    mine, theirs = col_i[...], both_i[256:512, :]
    put_side(slice(MARGIN, MARGIN + TILE), jnp.where(right, mine, theirs), jnp.where(right, theirs, mine), True)
    mine, theirs = c1_i[...], c2_i[...]
    put_side(pl.ds(own_rows, MARGIN), jnp.where(right, mine, theirs), jnp.where(right, theirs, mine), ok_own)
    mine, theirs = both_i[512:576, :], both_i[576:640, :]
    put_side(pl.ds(other_rows, MARGIN), jnp.where(right, theirs, mine), jnp.where(right, mine, theirs), ok_other)

    grad[...] = jnp.zeros(grad.shape, F32)
    lane = lax.broadcasted_iota(jnp.int32, (FRAME, FRAME), 1)

    def dot(a, b):
        return jnp.dot(a, b, preferred_element_type=F32)

    def slot_step(slot, carry):
        top = pos[slot, 0]
        turned = pos[slot, 1] + (WINDOW - MARGIN)
        first = (turned // 128) % 3
        second = (first + 1) % 3
        shift = turned % 128
        back_shift = (128 - shift) % 128
        head = lane >= shift
        patch = []
        for ri in range(2):
            a = ext[ri, first, pl.ds(top, FRAME), :]
            b = ext[ri, second, pl.ds(top, FRAME), :]
            patch.append(pltpu.roll(jnp.where(head, a, b), back_shift, 1))
        for m in range(MODES):
            p_real, p_imag = probes[m, 0:128, :], probes[m, 128:256, :]
            at = slice(m * 128, (m + 1) * 128)
            put_split(s1h, s1l, at, slice(0, 128), p_real * patch[0] - p_imag * patch[1])
            put_split(s1h, s1l, at, slice(128, 256), p_real * patch[1] + p_imag * patch[0])
        y = dot(s1h[...], tab[0]) + dot(s1h[...], tab[1]) + dot(s1l[...], tab[0])
        for m in range(MODES):
            at = slice(m * 128, (m + 1) * 128)
            put_split(s2h, s2l, slice(0, 128), at, y[at, 0:128])
            put_split(s2h, s2l, slice(128, 256), at, y[at, 128:256])
        z = dot(tab[2], s2h[...]) + dot(tab[3], s2h[...]) + dot(tab[2], s2l[...])
        zs[...] = z
        intensity = jnp.zeros((FRAME, FRAME), F32)
        for m in range(MODES):
            at = slice(m * 128, (m + 1) * 128)
            z_real, z_imag = z[0:128, at], z[128:256, at]
            intensity = intensity + (z_real * z_real + z_imag * z_imag)
        keep = 1.0 - amp[slot] * jnp.minimum(lax.rsqrt(intensity), 1.0)
        for m in range(MODES):
            at = slice(m * 128, (m + 1) * 128)
            put_split(s3h, s3l, slice(0, 128), at, zs[0:128, at] * keep)
            put_split(s3h, s3l, slice(128, 256), at, zs[128:256, at] * keep)
        u = dot(tab[0], s3h[...]) + dot(tab[1], s3h[...]) + dot(tab[0], s3l[...])
        for m in range(MODES):
            at = slice(m * 128, (m + 1) * 128)
            put_split(s4h, s4l, at, slice(0, 128), u[0:128, at])
            put_split(s4h, s4l, at, slice(128, 256), u[128:256, at])
        w = dot(s4h[...], tab[2]) + dot(s4h[...], tab[3]) + dot(s4l[...], tab[2])
        g_real = jnp.zeros((FRAME, FRAME), F32)
        g_imag = jnp.zeros((FRAME, FRAME), F32)
        for m in range(MODES):
            p_real, p_imag = probes[m, 0:128, :], probes[m, 128:256, :]
            at = slice(m * 128, (m + 1) * 128)
            b_real, b_imag = w[at, 0:128], w[at, 128:256]
            g_real = g_real + (p_real * b_real + p_imag * b_imag)
            g_imag = g_imag + (p_real * b_imag - p_imag * b_real)
        for ri, g in enumerate((g_real, g_imag)):
            g = pltpu.roll(g, shift, 1)
            grad[ri, first, pl.ds(top, FRAME), :] += jnp.where(head, g, 0.0)
            grad[ri, second, pl.ds(top, FRAME), :] += jnp.where(head, 0.0, g)
        return carry

    lax.fori_loop(0, cnt[0], slot_step, 0)

    for ri in range(2):
        for blk in range(2):
            cols = slice(blk * 128, (blk + 1) * 128)
            part_o[ri, :, cols] = obj[ri, :, cols] - STEP_SIZE * grad[ri, blk, MARGIN : MARGIN + TILE, :]
            row_o[pl.ds((ri * 2 + blk) * MARGIN, MARGIN), :] = grad[ri, blk, pl.ds(own_rows, MARGIN), :]
    col_o[...] = packed(grad[0, 2, MARGIN : MARGIN + TILE, :], grad[1, 2, MARGIN : MARGIN + TILE, :], right)
    corner_real, corner_imag = grad[0, 2, pl.ds(own_rows, MARGIN), :], grad[1, 2, pl.ds(own_rows, MARGIN), :]
    c1_o[...] = packed(corner_real, corner_imag, right)
    c2_o[...] = packed(corner_real, corner_imag, jnp.logical_not(right))


def fold_kernel(part, row_i, col_i, c1_i, c2_i, both, out):
    r, c, down, right = directions()
    rows_count, cols_count = lax.axis_size("row"), lax.axis_size("col")
    ok = {"down": r < rows_count - 1, "up": r > 0, "right": c < cols_count - 1, "left": c > 0}
    out[...] = part[...]

    def pick(flag, mine, theirs):
        return jnp.where(flag, mine, theirs)

    def scaled(flag, value):
        return jnp.where(flag, STEP_SIZE * value, 0.0)

    edges = {"up": slice(0, MARGIN), "down": slice(TILE - MARGIN, TILE)}
    for name, flag in (("up", jnp.logical_not(down)), ("down", down)):
        for ri in range(2):
            for blk in range(2):
                at = (ri * 2 + blk) * MARGIN
                piece = pick(flag, row_i[at : at + MARGIN, :], both[at : at + MARGIN, :])
                out[ri, edges[name], blk * 128 : (blk + 1) * 128] -= scaled(ok[name], piece)

    def take_side(rows, side, piece, flag):
        low = lanes_below(piece.shape)
        natural = low if side == "left" else jnp.logical_not(low)
        cols = slice(0, 128) if side == "left" else slice(128, 256)
        piece = scaled(flag, piece)
        out[0, rows, cols] -= jnp.where(natural, piece, 0.0)
        out[1, rows, cols] -= jnp.where(natural, pltpu.roll(piece, MARGIN, 1), 0.0)

    for side, flag in (("left", jnp.logical_not(right)), ("right", right)):
        take_side(slice(None), side, pick(flag, col_i[...], both[256:512, :]), ok[side])
        for name, vertical in (("up", jnp.logical_not(down)), ("down", down)):
            mine = pick(flag, c1_i[...], c2_i[...])
            theirs = pick(flag, both[576:640, :], both[512:576, :])
            take_side(edges[name], side, pick(vertical, mine, theirs), jnp.logical_and(ok[side], ok[name]))


def shape(*dims):
    return jax.ShapeDtypeStruct(dims, F32)


PIECES = (shape(256, 128), shape(256, 128), shape(64, 128), shape(64, 128))
VMEM = pl.BlockSpec(memory_space=pltpu.VMEM)
SMEM = pl.BlockSpec(memory_space=pltpu.SMEM)


def solution(mesh):
    tables = dft_tables()
    shape_of = dict(mesh.shape)

    def exchange(row, col, c1, c2):
        row = swap(row, shape_of, ((1, 0, 0), (2, 0, 0)))
        col = swap(col, shape_of, ((0, 1, 0), (0, 2, 0)))
        c1 = swap(c1, shape_of, ((1, 1, 0), (2, 2, 0)))
        c2 = swap(c2, shape_of, ((1, 2, 0), (2, 1, 0)))
        return row, col, c1, c2

    def with_pair(*arrays):
        return swap(jnp.concatenate(arrays, axis=0), shape_of, ((0, 0, 1), (0, 0, 1)))

    def per_device(object_field, probe_real, probe_imag, amplitude, positions, counts):
        row, col, c1, c2, probe = pl.pallas_call(
            pack_kernel,
            out_shape=PIECES + (shape(256, 128),),
            in_specs=[VMEM] * 3,
            out_specs=[VMEM] * 5,
            name="pack",
        )(object_field, probe_real, probe_imag)
        xprobe = swap(probe, shape_of, ((0, 0, 2), (0, 0, 2)))
        halo = exchange(row, col, c1, c2)
        pprobe = with_pair(probe)
        both = with_pair(*halo, xprobe)
        wide = pltpu.VMEM((512, 256), BF16)
        tall = pltpu.VMEM((256, 512), BF16)
        part, *margins = pl.pallas_call(
            main_kernel,
            out_shape=(shape(2, TILE, TILE),) + PIECES,
            in_specs=[SMEM, SMEM] + [VMEM] * 11,
            out_specs=[VMEM] * 5,
            scratch_shapes=[
                pltpu.VMEM((2, 3, WINDOW, 128), F32),
                pltpu.VMEM((2, 3, WINDOW, 128), F32),
                pltpu.VMEM((MODES, 256, 128), F32),
                wide, wide, tall, tall,
                pltpu.VMEM((256, 512), F32),
                tall, tall, wide, wide,
            ],
            name="frames",
        )(positions[0, 0], counts[0], object_field, *halo, probe, xprobe, pprobe, both, amplitude[0, 0], tables)
        margins = exchange(*margins)
        both = with_pair(*margins)
        return pl.pallas_call(
            fold_kernel,
            out_shape=shape(2, TILE, TILE),
            in_specs=[VMEM] * 6,
            out_specs=VMEM,
            name="fold",
        )(part, *margins, both)

    in_specs = (
        P(None, "row", "col"),
        P("mode", None, None),
        P("mode", None, None),
        P("row", "col", None, None, None),
        P("row", "col", None, None),
        P("row", "col"),
    )
    return jax.shard_map(per_device, mesh=mesh, in_specs=in_specs, out_specs=P(None, "row", "col"), check_vma=False)
```

```python
import jax
import jax.numpy as jnp
import ml_dtypes
import numpy as np
from jax import lax
from jax.experimental import pallas as pl
from jax.experimental.pallas import tpu as pltpu
from jax.sharding import PartitionSpec as P

FRAME = 128
MARGIN = 64
SLOTS = 8
MODES = 4
TILE = 256
WINDOW = TILE + 2 * MARGIN
STEP_SIZE = 0.25
AXES = ("row", "col", "mode")
F32 = jnp.float32
BF16 = jnp.bfloat16


def dft_tables():
    n = np.arange(FRAME)
    angle = 2.0 * np.pi * ((n[:, None] * n[None, :]) % FRAME) / FRAME
    cosine, sine = np.cos(angle), np.sin(angle)
    right = np.block([[cosine, -sine], [sine, cosine]])
    left = right.T / FRAME

    def halves(table):
        table = table.astype(np.float32)
        high = table.astype(ml_dtypes.bfloat16)
        low = (table - high.astype(np.float32)).astype(ml_dtypes.bfloat16)
        return high, low

    return np.stack(halves(right) + halves(left))


def partner(kind, index, count):
    if kind == 0:
        return index
    if kind == 1:
        return index ^ 1
    return (((index + 1) ^ 1) - 1) % count if index else count - 1


def swap(x, mesh_shape, by_core):
    rows, cols, modes = (mesh_shape[a] for a in AXES)
    pairs = []
    for r in range(rows):
        for c in range(cols):
            for m in range(modes):
                row_kind, col_kind, flip = by_core[m % 2]
                rr, cc = partner(row_kind, r, rows), partner(col_kind, c, cols)
                pairs.append(((r * cols + c) * modes + m, (rr * cols + cc) * modes + (m ^ flip)))
    return lax.ppermute(x, AXES, pairs)


def lanes_below(shape):
    return lax.broadcasted_iota(jnp.int32, shape, len(shape) - 1) < MARGIN


def directions():
    r, c, k = lax.axis_index("row"), lax.axis_index("col"), lax.axis_index("mode") % 2
    down = (r + k) % 2 == 0
    right = (c + k) % 2 == 0
    return r, c, down, right


def packed(real, imag, lower):
    low = lanes_below(real.shape)
    natural = low == lower
    return jnp.where(natural, real, pltpu.roll(imag, MARGIN, 1))


def pack_kernel(obj, pr, pi, row_o, col_o, c1_o, c2_o, probe_o):
    _, _, down, right = directions()
    start = pl.multiple_of(jnp.where(down, TILE - MARGIN, 0), MARGIN)
    for ri in range(2):
        for blk in range(2):
            row_o[pl.ds((ri * 2 + blk) * MARGIN, MARGIN), :] = obj[ri, pl.ds(start, MARGIN), pl.ds(blk * 128, 128)]

    def side(rows, to_right):
        real = jnp.where(to_right, obj[0, rows, 128:256], obj[0, rows, 0:128])
        imag = jnp.where(to_right, obj[1, rows, 128:256], obj[1, rows, 0:128])
        return packed(real, imag, jnp.logical_not(to_right))

    col_o[...] = side(slice(None), right)
    c1_o[...] = side(pl.ds(start, MARGIN), right)
    c2_o[...] = side(pl.ds(start, MARGIN), jnp.logical_not(right))
    probe_o[0:128, :] = pr[0]
    probe_o[128:256, :] = pi[0]


def put_split(high, low, rows, cols, value):
    h = value.astype(BF16)
    high[rows, cols] = h
    low[rows, cols] = (value - h.astype(F32)).astype(BF16)


def main_kernel(
    pos, cnt, obj, row_i, col_i, c1_i, c2_i, probe_i, xprobe_i, pprobe_i, both_i, amp, tab,
    centre_o, own_o, other_o,
    ext, grad, probes, s1h, s1l, s2h, s2l, zs, s3h, s3l, s4h, s4l,
):
    r, c, down, right = directions()
    member = lax.axis_index("mode")
    core = member % 2
    rows_count, cols_count = lax.axis_size("row"), lax.axis_size("col")
    ok_down, ok_up = r < rows_count - 1, r > 0
    ok_right, ok_left = c < cols_count - 1, c > 0

    probes[member] = probe_i[...]
    probes[member ^ 2] = xprobe_i[...]
    probes[member ^ 1] = pprobe_i[...]
    probes[member ^ 3] = both_i[pl.ds(640, 256), :]

    for ri in range(2):
        for blk in range(2):
            ext[ri, blk, MARGIN : MARGIN + TILE, :] = obj[ri, :, blk * 128 : (blk + 1) * 128]
    own_rows = pl.multiple_of(jnp.where(down, MARGIN + TILE, 0), MARGIN)
    other_rows = pl.multiple_of(jnp.where(down, 0, MARGIN + TILE), MARGIN)
    ok_own = jnp.where(down, ok_down, ok_up)
    ok_other = jnp.where(down, ok_up, ok_down)
    for ri in range(2):
        for blk in range(2):
            at = (ri * 2 + blk) * MARGIN
            ext[ri, blk, pl.ds(own_rows, MARGIN), :] = jnp.where(ok_own, row_i[at : at + MARGIN, :], 0.0)
            ext[ri, blk, pl.ds(other_rows, MARGIN), :] = jnp.where(ok_other, both_i[at : at + MARGIN, :], 0.0)

    def put_side(rows, from_right, from_left, ok):
        low = lanes_below(from_right.shape)
        from_right = jnp.where(jnp.logical_and(ok, ok_right), from_right, 0.0)
        from_left = jnp.where(jnp.logical_and(ok, ok_left), from_left, 0.0)
        ext[0, 2, rows, :] = jnp.where(low, from_right, from_left)
        ext[1, 2, rows, :] = pltpu.roll(jnp.where(low, from_left, from_right), MARGIN, 1)

    mine, theirs = col_i[...], both_i[256:512, :]
    put_side(slice(MARGIN, MARGIN + TILE), jnp.where(right, mine, theirs), jnp.where(right, theirs, mine), True)
    mine, theirs = c1_i[...], c2_i[...]
    put_side(pl.ds(own_rows, MARGIN), jnp.where(right, mine, theirs), jnp.where(right, theirs, mine), ok_own)
    mine, theirs = both_i[512:576, :], both_i[576:640, :]
    put_side(pl.ds(other_rows, MARGIN), jnp.where(right, theirs, mine), jnp.where(right, mine, theirs), ok_other)

    grad[...] = jnp.zeros(grad.shape, F32)
    lane = lax.broadcasted_iota(jnp.int32, (FRAME, FRAME), 1)

    def dot(a, b):
        return jnp.dot(a, b, preferred_element_type=F32)

    def slot_step(turn, carry):
        slot = 2 * turn + core
        top = pos[0, 0, 0, slot]
        turned = pos[0, 0, 1, slot] + (WINDOW - MARGIN)
        first = (turned // 128) % 3
        second = (first + 1) % 3
        shift = turned % 128
        back_shift = (128 - shift) % 128
        head = lane >= shift
        patch = []
        for ri in range(2):
            a = ext[ri, first, pl.ds(top, FRAME), :]
            b = ext[ri, second, pl.ds(top, FRAME), :]
            patch.append(pltpu.roll(jnp.where(head, a, b), back_shift, 1))
        for m in range(MODES):
            p_real, p_imag = probes[m, 0:128, :], probes[m, 128:256, :]
            at = slice(m * 128, (m + 1) * 128)
            put_split(s1h, s1l, at, slice(0, 128), p_real * patch[0] - p_imag * patch[1])
            put_split(s1h, s1l, at, slice(128, 256), p_real * patch[1] + p_imag * patch[0])
        y = dot(s1h[...], tab[0]) + dot(s1h[...], tab[1]) + dot(s1l[...], tab[0])
        for m in range(MODES):
            at = slice(m * 128, (m + 1) * 128)
            put_split(s2h, s2l, slice(0, 128), at, y[at, 0:128])
            put_split(s2h, s2l, slice(128, 256), at, y[at, 128:256])
        z = dot(tab[2], s2h[...]) + dot(tab[3], s2h[...]) + dot(tab[2], s2l[...])
        zs[...] = z
        intensity = jnp.zeros((FRAME, FRAME), F32)
        for m in range(MODES):
            at = slice(m * 128, (m + 1) * 128)
            z_real, z_imag = z[0:128, at], z[128:256, at]
            intensity = intensity + (z_real * z_real + z_imag * z_imag)
        keep = 1.0 - amp[slot] * jnp.minimum(lax.rsqrt(intensity), 1.0)
        for m in range(MODES):
            at = slice(m * 128, (m + 1) * 128)
            put_split(s3h, s3l, slice(0, 128), at, zs[0:128, at] * keep)
            put_split(s3h, s3l, slice(128, 256), at, zs[128:256, at] * keep)
        u = dot(tab[0], s3h[...]) + dot(tab[1], s3h[...]) + dot(tab[0], s3l[...])
        for m in range(MODES):
            at = slice(m * 128, (m + 1) * 128)
            put_split(s4h, s4l, at, slice(0, 128), u[0:128, at])
            put_split(s4h, s4l, at, slice(128, 256), u[128:256, at])
        w = dot(s4h[...], tab[2]) + dot(s4h[...], tab[3]) + dot(s4l[...], tab[2])
        g_real = jnp.zeros((FRAME, FRAME), F32)
        g_imag = jnp.zeros((FRAME, FRAME), F32)
        for m in range(MODES):
            p_real, p_imag = probes[m, 0:128, :], probes[m, 128:256, :]
            at = slice(m * 128, (m + 1) * 128)
            b_real, b_imag = w[at, 0:128], w[at, 128:256]
            g_real = g_real + (p_real * b_real + p_imag * b_imag)
            g_imag = g_imag + (p_real * b_imag - p_imag * b_real)
        for ri, g in enumerate((g_real, g_imag)):
            g = pltpu.roll(g, shift, 1)
            grad[ri, first, pl.ds(top, FRAME), :] += jnp.where(head, g, 0.0)
            grad[ri, second, pl.ds(top, FRAME), :] += jnp.where(head, 0.0, g)
        return carry

    lax.fori_loop(0, (cnt[0, 0] + 1 - core) // 2, slot_step, 0)

    for ri in range(2):
        for blk in range(2):
            at = (ri * 2 + blk) * TILE
            centre_o[at : at + TILE, :] = grad[ri, blk, MARGIN : MARGIN + TILE, :]
    side_real, side_imag = grad[0, 2, MARGIN : MARGIN + TILE, :], grad[1, 2, MARGIN : MARGIN + TILE, :]
    for out, rows, to_right in ((own_o, own_rows, right), (other_o, other_rows, jnp.logical_not(right))):
        for ri in range(2):
            for blk in range(2):
                out[pl.ds((ri * 2 + blk) * MARGIN, MARGIN), :] = grad[ri, blk, pl.ds(rows, MARGIN), :]
        out[256:512, :] = packed(side_real, side_imag, to_right)
        corner_real, corner_imag = grad[0, 2, pl.ds(rows, MARGIN), :], grad[1, 2, pl.ds(rows, MARGIN), :]
        out[512:576, :] = packed(corner_real, corner_imag, to_right)
        out[576:640, :] = packed(corner_real, corner_imag, jnp.logical_not(to_right))


def join_kernel(own, other, row_o, col_o, c1_o, c2_o):
    row_o[...] = own[0:256, :] + other[0:256, :]
    col_o[...] = own[256:512, :] + other[256:512, :]
    c1_o[...] = own[512:576, :] + other[512:576, :]
    c2_o[...] = own[576:640, :] + other[576:640, :]


def fold_kernel(obj, centre, pcentre, row_i, col_i, c1_i, c2_i, both, out):
    r, c, down, right = directions()
    rows_count, cols_count = lax.axis_size("row"), lax.axis_size("col")
    ok = {"down": r < rows_count - 1, "up": r > 0, "right": c < cols_count - 1, "left": c > 0}
    for ri in range(2):
        for blk in range(2):
            at = slice((ri * 2 + blk) * TILE, (ri * 2 + blk + 1) * TILE)
            cols = slice(blk * 128, (blk + 1) * 128)
            out[ri, :, cols] = obj[ri, :, cols] - STEP_SIZE * (centre[at, :] + pcentre[at, :])

    def pick(flag, mine, theirs):
        return jnp.where(flag, mine, theirs)

    def scaled(flag, value):
        return jnp.where(flag, STEP_SIZE * value, 0.0)

    edges = {"up": slice(0, MARGIN), "down": slice(TILE - MARGIN, TILE)}
    for name, flag in (("up", jnp.logical_not(down)), ("down", down)):
        for ri in range(2):
            for blk in range(2):
                at = (ri * 2 + blk) * MARGIN
                piece = pick(flag, row_i[at : at + MARGIN, :], both[at : at + MARGIN, :])
                out[ri, edges[name], blk * 128 : (blk + 1) * 128] -= scaled(ok[name], piece)

    def take_side(rows, side, piece, flag):
        low = lanes_below(piece.shape)
        natural = low if side == "left" else jnp.logical_not(low)
        cols = slice(0, 128) if side == "left" else slice(128, 256)
        piece = scaled(flag, piece)
        out[0, rows, cols] -= jnp.where(natural, piece, 0.0)
        out[1, rows, cols] -= jnp.where(natural, pltpu.roll(piece, MARGIN, 1), 0.0)

    for side, flag in (("left", jnp.logical_not(right)), ("right", right)):
        take_side(slice(None), side, pick(flag, col_i[...], both[256:512, :]), ok[side])
        for name, vertical in (("up", jnp.logical_not(down)), ("down", down)):
            mine = pick(flag, c1_i[...], c2_i[...])
            theirs = pick(flag, both[576:640, :], both[512:576, :])
            take_side(edges[name], side, pick(vertical, mine, theirs), jnp.logical_and(ok[side], ok[name]))


def shape(*dims):
    return jax.ShapeDtypeStruct(dims, F32)


PIECES = (shape(256, 128), shape(256, 128), shape(64, 128), shape(64, 128))
VMEM = pl.BlockSpec(memory_space=pltpu.VMEM)
SMEM = pl.BlockSpec(memory_space=pltpu.SMEM)
SMALL = pltpu.CompilerParams(vmem_limit_bytes=8 << 20)


def solution(mesh):
    tables = dft_tables()
    shape_of = dict(mesh.shape)

    def exchange(row, col, c1, c2):
        row = swap(row, shape_of, ((1, 0, 0), (2, 0, 0)))
        col = swap(col, shape_of, ((0, 1, 0), (0, 2, 0)))
        c1 = swap(c1, shape_of, ((1, 1, 0), (2, 2, 0)))
        c2 = swap(c2, shape_of, ((1, 2, 0), (2, 1, 0)))
        return row, col, c1, c2

    def with_pair(*arrays):
        return swap(jnp.concatenate(arrays, axis=0), shape_of, ((0, 0, 1), (0, 0, 1)))

    def per_device(object_field, probe_real, probe_imag, amplitude, positions, counts):
        row, col, c1, c2, probe = pl.pallas_call(
            pack_kernel,
            out_shape=PIECES + (shape(256, 128),),
            in_specs=[VMEM] * 3,
            out_specs=[VMEM] * 5,
            compiler_params=SMALL,
            name="pack",
        )(object_field, probe_real, probe_imag)
        xprobe = swap(probe, shape_of, ((0, 0, 2), (0, 0, 2)))
        halo = exchange(row, col, c1, c2)
        pprobe = with_pair(probe)
        both = with_pair(*halo, xprobe)
        wide = pltpu.VMEM((512, 256), BF16)
        tall = pltpu.VMEM((256, 512), BF16)
        centre, own, other = pl.pallas_call(
            main_kernel,
            out_shape=(shape(4 * TILE, 128), shape(640, 128), shape(640, 128)),
            in_specs=[SMEM, SMEM] + [VMEM] * 11,
            out_specs=[VMEM] * 3,
            scratch_shapes=[
                pltpu.VMEM((2, 3, WINDOW, 128), F32),
                pltpu.VMEM((2, 3, WINDOW, 128), F32),
                pltpu.VMEM((MODES, 256, 128), F32),
                wide, wide, tall, tall,
                pltpu.VMEM((256, 512), F32),
                tall, tall, wide, wide,
            ],
            compiler_params=pltpu.CompilerParams(vmem_limit_bytes=20 << 20),
            name="frames",
        )(jnp.swapaxes(positions, 2, 3), counts, object_field, *halo, probe, xprobe, pprobe, both, amplitude[0, 0], tables)
        other = with_pair(other)
        pcentre = with_pair(centre)
        margins = pl.pallas_call(
            join_kernel,
            out_shape=PIECES,
            in_specs=[VMEM] * 2,
            out_specs=[VMEM] * 4,
            compiler_params=SMALL,
            name="join",
        )(own, other)
        margins = exchange(*margins)
        both = with_pair(*margins)
        return pl.pallas_call(
            fold_kernel,
            out_shape=shape(2, TILE, TILE),
            in_specs=[VMEM] * 8,
            out_specs=VMEM,
            compiler_params=SMALL,
            name="fold",
        )(object_field, centre, pcentre, *margins, both)

    in_specs = (
        P(None, "row", "col"),
        P("mode", None, None),
        P("mode", None, None),
        P("row", "col", None, None, None),
        P("row", "col", None, None),
        P("row", "col"),
    )
    return jax.shard_map(per_device, mesh=mesh, in_specs=in_specs, out_specs=P(None, "row", "col"), check_vma=False)
```

```python
import jax
import jax.numpy as jnp
import ml_dtypes
import numpy as np
from jax import lax
from jax.experimental import pallas as pl
from jax.experimental.pallas import tpu as pltpu
from jax.sharding import PartitionSpec as P

FRAME = 128
MARGIN = 64
SLOTS = 8
MODES = 4
TILE = 256
WINDOW = TILE + 2 * MARGIN
STEP_SIZE = 0.25
TOGETHER = 4
ORDER = 1
AXES = ("row", "col", "mode")
F32 = jnp.float32
BF16 = jnp.bfloat16


def dft_tables():
    n = np.arange(FRAME)
    angle = 2.0 * np.pi * ((n[:, None] * n[None, :]) % FRAME) / FRAME
    cosine, sine = np.cos(angle), np.sin(angle)
    right = np.block([[cosine, -sine], [sine, cosine]])
    left = right.T / FRAME

    def halves(table):
        table = table.astype(np.float32)
        high = table.astype(ml_dtypes.bfloat16)
        low = (table - high.astype(np.float32)).astype(ml_dtypes.bfloat16)
        return high, low

    return np.stack(halves(right) + halves(left))


def partner(kind, index, count):
    if kind == 0:
        return index
    if kind == 1:
        return index ^ 1
    return (((index + 1) ^ 1) - 1) % count if index else count - 1


def swap(x, mesh_shape, by_core):
    rows, cols, modes = (mesh_shape[a] for a in AXES)
    pairs = []
    for r in range(rows):
        for c in range(cols):
            for m in range(modes):
                row_kind, col_kind, flip = by_core[m % 2]
                rr, cc = partner(row_kind, r, rows), partner(col_kind, c, cols)
                pairs.append(((r * cols + c) * modes + m, (rr * cols + cc) * modes + (m ^ flip)))
    return lax.ppermute(x, AXES, pairs)


def lanes_below(shape):
    return lax.broadcasted_iota(jnp.int32, shape, len(shape) - 1) < MARGIN


def directions():
    r, c, k = lax.axis_index("row"), lax.axis_index("col"), lax.axis_index("mode") % 2
    down = (r + k) % 2 == 0
    right = (c + k) % 2 == 0
    return r, c, down, right


def vertical_starts(r, above, below):
    even = r % 2 == 0
    near, far = jnp.where(even, below, above), jnp.where(even, above, below)
    return pl.multiple_of(near, MARGIN), pl.multiple_of(far, MARGIN)


def packed(real, imag, lower):
    low = lanes_below(real.shape)
    natural = low == lower
    return jnp.where(natural, real, pltpu.roll(imag, MARGIN, 1))


def pack_kernel(obj, row_o, col_o, c1_o, c2_o):
    r, _, down, right = directions()
    start = pl.multiple_of(jnp.where(down, TILE - MARGIN, 0), MARGIN)
    near, far = vertical_starts(r, 0, TILE - MARGIN)
    for ri in range(2):
        for blk in range(2):
            row_o[pl.ds((ri * 2 + blk) * MARGIN, MARGIN), :] = obj[ri, pl.ds(start, MARGIN), pl.ds(blk * 128, 128)]

    def side(rows, to_right):
        real = jnp.where(to_right, obj[0, rows, 128:256], obj[0, rows, 0:128])
        imag = jnp.where(to_right, obj[1, rows, 128:256], obj[1, rows, 0:128])
        return packed(real, imag, jnp.logical_not(to_right))

    col_o[...] = side(slice(None), right)
    c1_o[...] = side(pl.ds(near, MARGIN), right)
    c2_o[...] = side(pl.ds(far, MARGIN), jnp.logical_not(right))


def main_kernel(
    pos, cnt, obj, row_i, col_i, c1_i, c2_i, probe_i, xprobe_i, pair_i, amp, tab,
    centre_o, own_o, other_o,
    ext, grad, probes,
):
    r, c, down, right = directions()
    member = lax.axis_index("mode")
    core = member % 2
    rows_count, cols_count = lax.axis_size("row"), lax.axis_size("col")
    ok_down, ok_up = r < rows_count - 1, r > 0
    ok_right, ok_left = c < cols_count - 1, c > 0

    probes[member] = probe_i[...]
    probes[member ^ 2] = xprobe_i[...]
    probes[member ^ 1] = pair_i[256:512, :]
    probes[member ^ 3] = pair_i[0:256, :]
    both_i = pair_i.at[512:1152, :]

    for ri in range(2):
        for blk in range(2):
            ext[ri, blk, MARGIN : MARGIN + TILE, :] = obj[ri, :, blk * 128 : (blk + 1) * 128]
    own_rows = pl.multiple_of(jnp.where(down, MARGIN + TILE, 0), MARGIN)
    other_rows = pl.multiple_of(jnp.where(down, 0, MARGIN + TILE), MARGIN)
    ok_own = jnp.where(down, ok_down, ok_up)
    ok_other = jnp.where(down, ok_up, ok_down)
    for ri in range(2):
        for blk in range(2):
            at = (ri * 2 + blk) * MARGIN
            ext[ri, blk, pl.ds(own_rows, MARGIN), :] = jnp.where(ok_own, row_i[at : at + MARGIN, :], 0.0)
            ext[ri, blk, pl.ds(other_rows, MARGIN), :] = jnp.where(ok_other, both_i[at : at + MARGIN, :], 0.0)

    def put_side(rows, from_right, from_left, ok):
        low = lanes_below(from_right.shape)
        from_right = jnp.where(jnp.logical_and(ok, ok_right), from_right, 0.0)
        from_left = jnp.where(jnp.logical_and(ok, ok_left), from_left, 0.0)
        ext[0, 2, rows, :] = jnp.where(low, from_right, from_left)
        ext[1, 2, rows, :] = pltpu.roll(jnp.where(low, from_left, from_right), MARGIN, 1)

    mine, theirs = col_i[...], both_i[256:512, :]
    put_side(slice(MARGIN, MARGIN + TILE), jnp.where(right, mine, theirs), jnp.where(right, theirs, mine), True)
    near, far = vertical_starts(r, 0, MARGIN + TILE)
    even = r % 2 == 0
    mine, theirs = c1_i[...], both_i[512:576, :]
    ok = jnp.where(even, ok_down, ok_up)
    put_side(pl.ds(near, MARGIN), jnp.where(right, mine, theirs), jnp.where(right, theirs, mine), ok)
    mine, theirs = c2_i[...], both_i[576:640, :]
    ok = jnp.where(even, ok_up, ok_down)
    put_side(pl.ds(far, MARGIN), jnp.where(right, theirs, mine), jnp.where(right, mine, theirs), ok)

    grad[...] = jnp.zeros(grad.shape, F32)
    lane = lax.broadcasted_iota(jnp.int32, (FRAME, FRAME), 1)

    def dot(a, b):
        return jnp.dot(a, b, preferred_element_type=F32)

    def split(value):
        high = value.astype(BF16)
        return high, (value - high.astype(F32)).astype(BF16)

    def times_table(value, at):
        high, low = split(value)
        return dot(high, tab[at]) + dot(high, tab[at + 1]) + dot(low, tab[at])

    def table_times(at, value):
        high, low = split(value)
        return dot(tab[at], high) + dot(tab[at + 1], high) + dot(tab[at], low)

    def beside(values):
        return jnp.concatenate(values, axis=1)

    def above(values):
        return jnp.concatenate(values, axis=0)

    blocks = [slice(m * 128, (m + 1) * 128) for m in range(MODES)]

    def enter(slot):
        top = pos[slot, 0]
        turned = pos[slot, 1] + (WINDOW - MARGIN)
        first = (turned // 128) % 3
        second = (first + 1) % 3
        shift = turned % 128
        head = lane >= shift
        patch = []
        for ri in range(2):
            a = ext[ri, first, pl.ds(top, FRAME), :]
            b = ext[ri, second, pl.ds(top, FRAME), :]
            patch.append(pltpu.roll(jnp.where(head, a, b), (128 - shift) % 128, 1))
        exits = []
        for m in range(MODES):
            p_real, p_imag = probes[m, 0:128, :], probes[m, 128:256, :]
            exits.append(beside([p_real * patch[0] - p_imag * patch[1], p_real * patch[1] + p_imag * patch[0]]))
        return slot, top, first, second, shift, head, above(exits)

    def forward(state):
        y = times_table(state[-1], 0)
        y = beside([above([y[at, 0:128], y[at, 128:256]]) for at in blocks])
        z = table_times(2, y)
        return state[:-1] + (z,)

    def middle(state):
        slot, z = state[0], state[-1]
        intensity = jnp.zeros((FRAME, FRAME), F32)
        for at in blocks:
            z_real, z_imag = z[0:128, at], z[128:256, at]
            intensity = intensity + (z_real * z_real + z_imag * z_imag)
        keep = 1.0 - amp[slot] * jnp.minimum(lax.rsqrt(intensity), 1.0)
        z = beside([above([z[0:128, at] * keep, z[128:256, at] * keep]) for at in blocks])
        return state[:-1] + (z,)

    def inverse(state):
        z = state[-1]
        u = table_times(0, z)
        u = above([beside([u[0:128, at], u[128:256, at]]) for at in blocks])
        w = times_table(u, 2)
        return state[:-1] + (w,)

    def leave(state):
        slot, top, first, second, shift, head, w = state
        g_real = jnp.zeros((FRAME, FRAME), F32)
        g_imag = jnp.zeros((FRAME, FRAME), F32)
        for m, at in enumerate(blocks):
            p_real, p_imag = probes[m, 0:128, :], probes[m, 128:256, :]
            b_real, b_imag = w[at, 0:128], w[at, 128:256]
            g_real = g_real + (p_real * b_real + p_imag * b_imag)
            g_imag = g_imag + (p_real * b_imag - p_imag * b_real)
        counted = slot < cnt[0, 0]
        for ri, g in enumerate((g_real, g_imag)):
            g = pltpu.roll(jnp.where(counted, g, 0.0), shift, 1)
            grad[ri, first, pl.ds(top, FRAME), :] += jnp.where(head, g, 0.0)
            grad[ri, second, pl.ds(top, FRAME), :] += jnp.where(head, 0.0, g)

    def step(turn, carry):
        slots = [2 * (turn * TOGETHER + k) + core for k in range(TOGETHER)]
        stages = (enter, forward, middle, inverse, leave)
        states = list(slots)
        for t in range(TOGETHER + ORDER * (len(stages) - 1)):
            for n in range(len(stages)):
                k = t - ORDER * n
                if 0 <= k < TOGETHER:
                    states[k] = stages[n](states[k])
        return carry

    lax.fori_loop(0, SLOTS // 2 // TOGETHER, step, 0)

    for ri in range(2):
        for blk in range(2):
            at = (ri * 2 + blk) * TILE
            centre_o[at : at + TILE, :] = grad[ri, blk, MARGIN : MARGIN + TILE, :]
    side_real, side_imag = grad[0, 2, MARGIN : MARGIN + TILE, :], grad[1, 2, MARGIN : MARGIN + TILE, :]
    for out, rows, to_right in ((own_o, own_rows, right), (other_o, other_rows, jnp.logical_not(right))):
        for ri in range(2):
            for blk in range(2):
                out[pl.ds((ri * 2 + blk) * MARGIN, MARGIN), :] = grad[ri, blk, pl.ds(rows, MARGIN), :]
        out[256:512, :] = packed(side_real, side_imag, to_right)
        for at, start, turn in ((512, near, to_right), (576, far, jnp.logical_not(to_right))):
            corner_real, corner_imag = grad[0, 2, pl.ds(start, MARGIN), :], grad[1, 2, pl.ds(start, MARGIN), :]
            out[at : at + MARGIN, :] = packed(corner_real, corner_imag, turn)


def join_kernel(own, other, row_o, col_o, c1_o, c2_o):
    row_o[...] = own[0:256, :] + other[0:256, :]
    col_o[...] = own[256:512, :] + other[256:512, :]
    c1_o[...] = own[512:576, :] + other[512:576, :]
    c2_o[...] = own[576:640, :] + other[576:640, :]


def fold_kernel(obj, centre, pcentre, row_i, col_i, c1_i, c2_i, both, out):
    r, c, down, right = directions()
    rows_count, cols_count = lax.axis_size("row"), lax.axis_size("col")
    ok = {"down": r < rows_count - 1, "up": r > 0, "right": c < cols_count - 1, "left": c > 0}
    for ri in range(2):
        for blk in range(2):
            at = slice((ri * 2 + blk) * TILE, (ri * 2 + blk + 1) * TILE)
            cols = slice(blk * 128, (blk + 1) * 128)
            out[ri, :, cols] = obj[ri, :, cols] - STEP_SIZE * (centre[at, :] + pcentre[at, :])

    def pick(flag, mine, theirs):
        return jnp.where(flag, mine, theirs)

    def scaled(flag, value):
        return jnp.where(flag, STEP_SIZE * value, 0.0)

    edges = {"up": slice(0, MARGIN), "down": slice(TILE - MARGIN, TILE)}
    for name, flag in (("up", jnp.logical_not(down)), ("down", down)):
        for ri in range(2):
            for blk in range(2):
                at = (ri * 2 + blk) * MARGIN
                piece = pick(flag, row_i[at : at + MARGIN, :], both[at : at + MARGIN, :])
                out[ri, edges[name], blk * 128 : (blk + 1) * 128] -= scaled(ok[name], piece)

    def take_side(rows, side, piece, flag):
        low = lanes_below(piece.shape)
        natural = low if side == "left" else jnp.logical_not(low)
        cols = slice(0, 128) if side == "left" else slice(128, 256)
        piece = scaled(flag, piece)
        out[0, rows, cols] -= jnp.where(natural, piece, 0.0)
        out[1, rows, cols] -= jnp.where(natural, pltpu.roll(piece, MARGIN, 1), 0.0)

    for side, flag in (("left", jnp.logical_not(right)), ("right", right)):
        take_side(slice(None), side, pick(flag, col_i[...], both[256:512, :]), ok[side])
        near = pick(flag, c1_i[...], both[512:576, :])
        far = pick(flag, both[576:640, :], c2_i[...])
        for name, is_near in (("up", r % 2 == 1), ("down", r % 2 == 0)):
            take_side(edges[name], side, pick(is_near, near, far), jnp.logical_and(ok[side], ok[name]))


def shape(*dims):
    return jax.ShapeDtypeStruct(dims, F32)


PIECES = (shape(256, 128), shape(256, 128), shape(64, 128), shape(64, 128))
VMEM = pl.BlockSpec(memory_space=pltpu.VMEM)
SMEM = pl.BlockSpec(memory_space=pltpu.SMEM)
SMALL = pltpu.CompilerParams(vmem_limit_bytes=8 << 20)


def solution(mesh):
    tables = dft_tables()
    shape_of = dict(mesh.shape)

    def exchange(row, col, c1, c2):
        row = swap(row, shape_of, ((1, 0, 0), (2, 0, 0)))
        col = swap(col, shape_of, ((0, 1, 0), (0, 2, 0)))
        c1 = swap(c1, shape_of, ((1, 1, 0), (1, 2, 0)))
        c2 = swap(c2, shape_of, ((2, 2, 0), (2, 1, 0)))
        return row, col, c1, c2

    def with_pair(*arrays):
        return swap(jnp.concatenate(arrays, axis=0), shape_of, ((0, 0, 1), (0, 0, 1)))

    def per_device(object_field, probe_real, probe_imag, amplitude, positions, counts):
        probe = jnp.concatenate([probe_real[0], probe_imag[0]], axis=0)
        xprobe = swap(probe, shape_of, ((1, 0, 2), (1, 0, 2)))
        row, col, c1, c2 = pl.pallas_call(
            pack_kernel,
            out_shape=PIECES,
            in_specs=[VMEM],
            out_specs=[VMEM] * 4,
            compiler_params=SMALL,
            name="pack",
        )(object_field)
        halo = exchange(row, col, c1, c2)
        both = with_pair(xprobe, probe, *halo)
        centre, own, other = pl.pallas_call(
            main_kernel,
            out_shape=(shape(4 * TILE, 128), shape(640, 128), shape(640, 128)),
            in_specs=[SMEM, SMEM] + [VMEM] * 10,
            out_specs=[VMEM] * 3,
            scratch_shapes=[
                pltpu.VMEM((2, 3, WINDOW, 128), F32),
                pltpu.VMEM((2, 3, WINDOW, 128), F32),
                pltpu.VMEM((MODES, 256, 128), F32),
            ],
            compiler_params=pltpu.CompilerParams(vmem_limit_bytes=20 << 20),
            name="frames",
        )(positions[0, 0], counts, object_field, *halo, probe, xprobe, both, amplitude[0, 0], tables)
        other = with_pair(other)
        pcentre = with_pair(centre)
        margins = pl.pallas_call(
            join_kernel,
            out_shape=PIECES,
            in_specs=[VMEM] * 2,
            out_specs=[VMEM] * 4,
            compiler_params=SMALL,
            name="join",
        )(own, other)
        margins = exchange(*margins)
        both = with_pair(*margins)
        return pl.pallas_call(
            fold_kernel,
            out_shape=shape(2, TILE, TILE),
            in_specs=[VMEM] * 8,
            out_specs=VMEM,
            compiler_params=SMALL,
            name="fold",
        )(object_field, centre, pcentre, *margins, both)

    in_specs = (
        P(None, "row", "col"),
        P("mode", None, None),
        P("mode", None, None),
        P("row", "col", None, None, None),
        P("row", "col", None, None),
        P("row", "col"),
    )
    return jax.shard_map(per_device, mesh=mesh, in_specs=in_specs, out_specs=P(None, "row", "col"), check_vma=False)
```
